32 devices in a mesh: seq: 8 (over z, y), rep: 4 (over x, core).
Axes of the slice: x: 2, y: 2, z: 4, core: 2. Of those that a mesh axis runs over, the one named last changes fastest.
Arguments:
- queries: bfloat16 [32, 32, 128], P('seq', 'rep'), may hold values from -48 to 48
- key_cache: bfloat16 [8, 16384, 128], P('rep', 'seq'), may hold values from -6 to 6
- value_cache: bfloat16 [8, 16384, 128], P('rep', 'seq'), may hold values from -6 to 6
- summary_keys: bfloat16 [8, 8, 128], P('rep', 'seq'), may hold values from -16 to 16
- summary_values: bfloat16 [8, 8, 128], P('rep', 'seq'), may hold values from -6 to 6
- owner_map: int32 [8], replicated, may hold values from 0 to 7, each once
- super_ids: int32 [32, 8, 4], P(None, 'rep'), may hold values from 0 to 7, as said below
- fine_ids: int32 [32, 8, 16], P(None, 'rep'), may hold values from 0 to 63, all different within a row
Outputs:
- attended: bfloat16 [32, 32, 128], P(('seq', 'rep'))
The draws below stay inside these ranges and needn't reach their ends.
Inputs may be any that keep to these rules, and one draw needn't show every extreme that they name: `super_ids`: each row names 4 different super-blocks; among the rows of one sender group (the 4 requests of one index of seq with the 2 key-value heads of one index of rep) no super-block is named more than 5 times, and in every such group some super-block is named exactly 5 times. `fine_ids`: each row names 16 different positions; position p is block p % 16 of super-block super_ids[r, g, p // 16]. `owner_map`: a permutation; slot q covers fine blocks q * 16 to q * 16 + 15 of the caches.
All inputs are finite; a program needn't handle non-finite values.
Results may differ from the reference program's by a relative error of at most 0.004.
Values may be sent and summed in bfloat16 or wider, within the bound.
A program may use at most 64 MiB of HBM per device.

```python
import math
import jax
import jax.numpy as jnp
from jax import lax

H = 32
KVH = 8
HD = 128
BLK = 128
SUPER = 16
REQ_DEV = 4
NSEL_SB = 4
NSEL_FB = 16
KVH_DEV = 2
NTOK = 16384
NSB = 8
REQUESTS = 32
CAP = 5


def draw_queries(key, part):
    random_part = jnp.clip(jax.random.normal(jax.random.fold_in(key, 11), (REQUESTS, H, HD), jnp.float32), -5.0, 5.0)
    return (3.0 * random_part).astype(jnp.bfloat16)


def draw_summary_keys(key, part):
    random_part = jnp.clip(jax.random.normal(jax.random.fold_in(key, 21), (KVH, NSB, HD), jnp.float32), -5.0, 5.0)
    return random_part.astype(jnp.bfloat16)


def draw_super_ids(key, part):
    seq_count = REQUESTS // REQ_DEV
    rep_count = KVH // KVH_DEV
    senders = seq_count * rep_count
    group_rows = REQ_DEV * KVH_DEV
    others = NSB - 1
    hottest = jax.random.randint(jax.random.fold_in(key, 31), (), 0, NSB)
    order_keys = jax.random.split(jax.random.fold_in(key, 32), senders)
    orders = jax.vmap(lambda single: jax.random.permutation(single, others))(order_keys)
    rank_keys = jax.random.split(jax.random.fold_in(key, 33), senders)
    row_rank = jax.vmap(lambda single: jax.random.permutation(single, group_rows))(rank_keys)
    position = (jnp.arange(group_rows)[:, None] * NSEL_SB + jnp.arange(NSEL_SB)[None, :]) % others
    picks = orders[:, position.reshape(-1)].reshape(senders, group_rows, NSEL_SB)
    picks = picks + (picks >= hottest).astype(picks.dtype)
    first = jnp.where(row_rank < CAP, hottest, picks[:, :, 0])
    picks = jnp.concatenate([first[:, :, None], picks[:, :, 1:]], axis=2)
    picks = picks.reshape(seq_count, rep_count, REQ_DEV, KVH_DEV, NSEL_SB)
    picks = jnp.transpose(picks, (0, 2, 1, 3, 4)).reshape(REQUESTS, KVH, NSEL_SB)
    return picks.astype(jnp.int32)


def block_scale(own_key, shape, shards, least, high):
    factor_of = 1.0
    for axis_at, blocks in shards:
        draws = jax.random.uniform(jax.random.fold_in(jax.random.fold_in(own_key, 6), axis_at), (blocks,), jnp.float32, least / len(shards), high / len(shards))
        factor_of = factor_of * jnp.repeat(jnp.exp(draws), shape[axis_at] // blocks).reshape((-1,) + (1,) * (len(shape) - 1 - axis_at))
    return factor_of


def different_ones(rng, rows, number_of, top, lift):
    ranking = jax.random.permutation(jax.random.fold_in(rng, 1), number_of)
    boost = ranking
    for power in range(3):
        boost = boost * boost // number_of
    boost = boost * lift // number_of
    tickets = jax.random.randint(jax.random.fold_in(rng, 2), (rows, number_of), 0, 4096) + boost
    fixed_rows = jax.random.permutation(jax.random.fold_in(rng, 3), rows)[jnp.arange(number_of) % rows]
    tickets = jnp.where(jnp.arange(rows)[:, None] == fixed_rows[None, :], 1 << 14, tickets)
    score = tickets * number_of + jnp.arange(number_of)
    return lax.top_k(score.astype(jnp.int32), top)[1].astype(jnp.int32)


def normal_values(own_key, dims, scale, limit, cuts=(), kind=jnp.bfloat16):
    drawn = jax.random.normal(own_key, dims, jnp.float32) * scale
    if len(cuts) > 0:
        drawn = block_scale(own_key, dims, cuts, -0.22, 0.18) * drawn
    return jnp.clip(drawn, min=-limit, max=limit).astype(kind)


def setup_inputs(seed: int = 0) -> dict:
    arg_keys = jax.random.split(jax.random.key(seed), 9)
    return {
        "queries": draw_queries(jax.random.fold_in(arg_keys[8], 71), 0),
        "key_cache": normal_values(arg_keys[1], (KVH, NTOK, HD), 1.0, 6.0, ((0, 4), (1, 8))),
        "value_cache": normal_values(arg_keys[2], (KVH, NTOK, HD), 1.0, 6.0, ((0, 4), (1, 8))),
        "summary_keys": draw_summary_keys(jax.random.fold_in(arg_keys[8], 71), 0),
        "summary_values": normal_values(arg_keys[4], (KVH, NSB, HD), 1.0, 6.0, ((0, 4), (1, 8))),
        "owner_map": jax.random.permutation(arg_keys[5], NSB).astype(jnp.int32),
        "super_ids": draw_super_ids(jax.random.fold_in(arg_keys[8], 71), 0),
        "fine_ids": different_ones(arg_keys[7], REQUESTS * KVH, NSEL_SB * SUPER, NSEL_FB, 2048).reshape((REQUESTS, KVH, NSEL_FB)),
    }


NEGATIVE = -1.0e30


def reference(queries, key_cache, value_cache, summary_keys, summary_values, owner_map, super_ids, fine_ids):
    kv_heads = key_cache.shape[0]
    head_dim = queries.shape[2]
    per_group = queries.shape[1] // kv_heads
    scaling = head_dim ** -0.5
    slots = owner_map[super_ids]
    picked = jnp.take_along_axis(slots, (fine_ids // SUPER).astype(jnp.int32), axis=2)
    chosen = (picked * SUPER + fine_ids % SUPER).astype(jnp.int32)
    key_blocks = key_cache.reshape(kv_heads, -1, BLK, head_dim)
    value_blocks = value_cache.reshape(kv_heads, -1, BLK, head_dim)
    slot_count = summary_keys.shape[1]
    head_index = jnp.arange(kv_heads, dtype=jnp.int32)[:, None]
    wide_keys = summary_keys.astype(jnp.float32)
    wide_values = summary_values.astype(jnp.float32)

    def attend(pieces):
        query, picked_blocks, picked_slots = pieces
        grouped = query.astype(jnp.float32).reshape(kv_heads, per_group, head_dim)
        fine_keys = key_blocks[head_index, picked_blocks].astype(jnp.float32).reshape(kv_heads, -1, head_dim)
        fine_values = value_blocks[head_index, picked_blocks].astype(jnp.float32).reshape(kv_heads, -1, head_dim)
        fine_scores = jnp.einsum("gqd,gtd->gqt", grouped, fine_keys, precision=lax.Precision.HIGHEST) * scaling
        kept = jnp.logical_not(jnp.any(picked_slots[:, :, None] == jnp.arange(slot_count, dtype=jnp.int32)[None, None, :], axis=1))
        coarse_scores = jnp.einsum("gqd,gsd->gqs", grouped, wide_keys, precision=lax.Precision.HIGHEST) * scaling + math.log(SUPER)
        coarse_scores = jnp.where(kept[:, None, :], coarse_scores, NEGATIVE)
        every_score = jnp.concatenate([fine_scores, coarse_scores], axis=2)
        highest = jnp.max(every_score, axis=2, keepdims=True)
        weights = jnp.exp(every_score - highest)
        joined_values = jnp.concatenate([fine_values, wide_values], axis=1)
        result = jnp.einsum("gqn,gnd->gqd", weights, joined_values, precision=lax.Precision.HIGHEST)
        result = result / jnp.sum(weights, axis=2)[..., None]
        return result.reshape(-1, head_dim).astype(jnp.bfloat16)

    return lax.map(attend, (queries, chosen, slots))
```

```python
import functools
import math

import jax
import jax.numpy as jnp
from jax import lax
from jax.experimental import pallas as pl
from jax.experimental.pallas import tpu as pltpu
from jax.sharding import PartitionSpec as P

BLK = 128
SUPER = 16
NEGATIVE = -1e30
LOG2E = math.log2(math.e)
CHUNK = 32
UNROLL_LIMIT = 64


def repeat(count, body):
    if count <= UNROLL_LIMIT:
        for step in range(count):
            body(step)
    else:

        def rolled(step, carry):
            body(step)
            return carry

        lax.fori_loop(0, count, rolled, 0)


def kernel(
    seq_size,
    rep_size,
    q_hbm,
    k_hbm,
    v_hbm,
    sk_hbm,
    sv_hbm,
    owner_hbm,
    super_hbm,
    fine_hbm,
    out_ref,
    q_own,
    k_ref,
    v_ref,
    sk_ref,
    sv_ref,
    owner_ref,
    super_ref,
    fine_ref,
    q_all,
    parts,
    landed,
    in_sems,
    kv_sems,
    q_send,
    q_recv,
    p_send,
    p_recv,
):
    my_seq = lax.axis_index("seq")
    my_rep = lax.axis_index("rep")
    devices = seq_size * rep_size
    me = my_seq * rep_size + my_rep
    own_rows, heads, head_dim = q_own.shape
    groups, tokens = k_ref.shape[:2]
    per_group = heads // groups
    slot_count = owner_ref.shape[0]
    requests = parts.shape[0]
    out_rows = out_ref.shape[0]
    blocks = tokens // BLK

    small = [
        pltpu.make_async_copy(src, dst, in_sems.at[i])
        for i, (src, dst) in enumerate(
            (
                (q_hbm, q_own),
                (owner_hbm, owner_ref),
                (super_hbm, super_ref),
                (fine_hbm, fine_ref),
                (sk_hbm, sk_ref),
                (sv_hbm, sv_ref),
            )
        )
    ]
    for copy in small:
        copy.start()
    big = []
    for g in range(groups):
        big.append(
            (
                pltpu.make_async_copy(k_hbm.at[g], k_ref.at[g], kv_sems.at[0, g]),
                pltpu.make_async_copy(v_hbm.at[g], v_ref.at[g], kv_sems.at[1, g]),
            )
        )
    for pair in big:
        for copy in pair:
            copy.start()

    barrier = pltpu.get_barrier_semaphore()

    def greet(step):
        other = lax.rem(me + step + 1, devices)
        pl.semaphore_signal(
            barrier,
            inc=1,
            device_id=(lax.div(other, rep_size), lax.rem(other, rep_size)),
            device_id_type=pl.DeviceIdType.MESH,
        )

    repeat(devices - 1, greet)

    for copy in small:
        copy.wait()
    upper = lax.broadcasted_iota(jnp.int32, (heads, head_dim), 0) < per_group
    first, second = [], []
    for r in range(0, own_rows, 2):
        even = q_own[r].astype(jnp.float32)
        odd = q_own[r + 1].astype(jnp.float32)
        first.append(jnp.where(upper, even, pltpu.roll(odd, per_group, 0)))
        second.append(jnp.where(upper, pltpu.roll(even, per_group, 0), odd))
    q_all[my_seq, 0] = jnp.concatenate(first, axis=0).astype(jnp.bfloat16)
    q_all[my_seq, 1] = jnp.concatenate(second, axis=0).astype(jnp.bfloat16)

    pl.semaphore_wait(barrier, devices - 1)

    def send_queries(step):
        other = lax.rem(my_seq + step + 1, seq_size)
        pltpu.make_async_remote_copy(
            src_ref=q_all.at[my_seq],
            dst_ref=q_all.at[my_seq],
            send_sem=q_send,
            recv_sem=q_recv,
            device_id=(other, my_rep),
            device_id_type=pl.DeviceIdType.MESH,
        ).start()

    repeat(seq_size - 1, send_queries)

    if slot_count <= UNROLL_LIMIT:
        here = jnp.int32(0)
        for j in range(slot_count):
            here = here + jnp.where(owner_ref[j] == my_seq, j, 0)
    else:
        here = lax.fori_loop(
            0, slot_count, lambda j, total: total + jnp.where(owner_ref[j] == my_seq, j, 0), jnp.int32(0)
        )
    here = here.astype(jnp.float32)

    rows = CHUNK * per_group
    row_of = lax.broadcasted_iota(jnp.int32, (rows, CHUNK), 0)
    low = lax.broadcasted_iota(jnp.int32, (rows, CHUNK), 1) * per_group
    expand = jnp.where((row_of >= low) & (row_of < low + per_group), 1.0, 0.0).astype(jnp.bfloat16)
    scaling = head_dim ** (-0.5) * LOG2E

    def selection(chunk, g):
        picked = pl.ds(chunk * CHUNK, CHUNK)
        fine = fine_ref[picked, g, :].astype(jnp.float32).astype(jnp.bfloat16)
        supers = super_ref[picked, g, :].astype(jnp.float32).astype(jnp.bfloat16)
        fine = jnp.dot(expand, fine, preferred_element_type=jnp.float32)
        supers = jnp.dot(expand, supers, preferred_element_type=jnp.float32)
        place = lax.broadcasted_iota(jnp.int32, supers.shape, 1).astype(jnp.float32) + 1.0
        place = jnp.sum(jnp.where(supers == here, place, 0.0), axis=1, keepdims=True)
        at = (fine - SUPER * (place - 1.0)).astype(jnp.int32)
        valid = (at >= 0) & (at < SUPER) & (place > 0.0)
        bit = jnp.left_shift(1, jnp.clip(at, 0, SUPER - 1)).astype(jnp.float32)
        bits = jnp.sum(jnp.where(valid, bit, 0.0), axis=1, keepdims=True).astype(jnp.int32)
        return place, bits

    def attend(chunk, g, place, bits):
        sources = CHUNK // own_rows
        query = q_all[pl.ds(chunk * sources, sources), g].reshape(rows, head_dim)
        bits = jnp.broadcast_to(bits, (rows, BLK))
        scores = lax.dot_general(
            query, k_ref[g], (((1,), (1,)), ((), ())), preferred_element_type=jnp.float32
        )
        masked = []
        for b in range(blocks):
            one = scores[:, b * BLK : (b + 1) * BLK]
            masked.append(jnp.where((bits & (1 << b)) != 0, one, NEGATIVE))
        peak = functools.reduce(jnp.maximum, masked)
        peak = jnp.max(peak, axis=1, keepdims=True)
        weights = [jnp.exp2((one - peak) * scaling) for one in masked]
        total = jnp.sum(functools.reduce(jnp.add, weights), axis=1, keepdims=True)
        packed = jnp.concatenate([one.astype(jnp.bfloat16) for one in weights], axis=1)
        summed = jnp.dot(packed, v_ref[g], preferred_element_type=jnp.float32)
        coarse = jnp.sum(
            query.astype(jnp.float32) * sk_ref[g].astype(jnp.float32), axis=1, keepdims=True
        )
        coarse = coarse * scaling + math.log2(SUPER)
        stat = jnp.where(place > 0.0, peak * scaling + jnp.log2(total), coarse)
        value = jnp.where(place > 0.0, summed / total, sv_ref[g].astype(jnp.float32))
        return value, jnp.broadcast_to(stat, (rows, head_dim))

    def regroup(both):
        a, b = both
        pairs = rows // heads
        a = a.reshape(pairs, heads, head_dim)
        b = b.reshape(pairs, heads, head_dim)
        top = lax.broadcasted_iota(jnp.int32, a.shape, 1) < per_group
        even = jnp.where(top, a, pltpu.roll(b, per_group, 1))
        odd = jnp.where(top, pltpu.roll(a, per_group, 1), b)
        return even, odd

    def owner_chunk(chunk, chosen=None):
        if chosen is None:
            chosen = [selection(chunk, g) for g in range(groups)]
        results = [attend(chunk, g, *chosen[g]) for g in range(groups)]
        values = regroup([value for value, _ in results])
        stats = regroup([stat for _, stat in results])
        lane = lax.broadcasted_iota(jnp.int32, values[0].shape, 2)
        for which in range(2):
            stat = stats[which]
            high = stat.astype(jnp.bfloat16).astype(jnp.float32)
            rest = stat - high
            middle = rest.astype(jnp.bfloat16).astype(jnp.float32)
            last = rest - middle
            split = jnp.where(lane == 0, high, jnp.where(lane == 1, middle, jnp.where(lane == 2, last, 0.0)))
            message = jnp.concatenate([values[which], split], axis=1).astype(jnp.bfloat16)
            for pair in range(rows // heads):
                parts[chunk * CHUNK + 2 * pair + which] = message[pair]

    def wait_queries():
        got = q_all.at[pl.ds(0, seq_size - 1)]
        pltpu.make_async_copy(got, got, q_recv).wait()

    if requests == CHUNK:
        chosen = [selection(0, g) for g in range(groups)]
        for pair in big:
            for copy in pair:
                copy.wait()
        wait_queries()
        owner_chunk(0, chosen)
    else:
        for pair in big:
            for copy in pair:
                copy.wait()
        wait_queries()

        def chunk_step(chunk, carry):
            owner_chunk(chunk)
            return carry

        lax.fori_loop(0, requests // CHUNK, chunk_step, 0)

    def send_part(step):
        other = lax.rem(me + step + 1, devices)
        pltpu.make_async_remote_copy(
            src_ref=parts.at[pl.ds(other * out_rows, out_rows)],
            dst_ref=landed.at[me],
            send_sem=p_send,
            recv_sem=p_recv,
            device_id=(lax.div(other, rep_size), lax.rem(other, rep_size)),
            device_id_type=pl.DeviceIdType.MESH,
        ).start()

    repeat(devices - 1, send_part)
    landed[me] = parts[pl.ds(me * out_rows, out_rows)]
    got = landed.at[pl.ds(0, devices - 1)]
    pltpu.make_async_copy(got, got, p_recv).wait()

    for i in range(out_rows):
        for p in range(rep_size):
            stats, values = [], []
            for s in range(seq_size):
                message = landed[s * rep_size + p, i].astype(jnp.float32)
                values.append(message[:heads])
                stats.append(jnp.sum(message[heads:], axis=1, keepdims=True))
            peak = functools.reduce(jnp.maximum, stats)
            factors = [jnp.exp2(stat - peak) for stat in stats]
            total = functools.reduce(jnp.add, factors)
            summed = functools.reduce(jnp.add, [f * v for f, v in zip(factors, values)])
            out_ref[i, p * heads : (p + 1) * heads] = (summed / total).astype(out_ref.dtype)

    sent = q_all.at[pl.ds(0, seq_size - 1)]
    pltpu.make_async_copy(sent, sent, q_send).wait()
    sent = landed.at[pl.ds(0, devices - 1)]
    pltpu.make_async_copy(sent, sent, p_send).wait()


def solution(mesh):
    seq_size = mesh.shape["seq"]
    rep_size = mesh.shape["rep"]

    def shards(queries, key_cache, value_cache, summary_keys, summary_values, owner_map, super_ids, fine_ids):
        own_rows, heads, head_dim = queries.shape
        groups, tokens = key_cache.shape[:2]
        requests = super_ids.shape[0]
        devices = seq_size * rep_size
        out_rows = own_rows // rep_size
        assert summary_keys.shape[1] == 1 and tokens == SUPER * BLK
        assert groups == 2 and heads == 8 and own_rows % rep_size == 0 and own_rows % 2 == 0
        assert requests % CHUNK == 0 and CHUNK % own_rows == 0
        per_source = own_rows * heads // groups
        hbm = pl.BlockSpec(memory_space=pltpu.HBM)
        return pl.pallas_call(
            functools.partial(kernel, seq_size, rep_size),
            out_shape=jax.ShapeDtypeStruct((out_rows, rep_size * heads, head_dim), jnp.bfloat16),
            in_specs=[hbm] * 8,
            out_specs=pl.BlockSpec(memory_space=pltpu.VMEM),
            scratch_shapes=[
                pltpu.VMEM(queries.shape, queries.dtype),
                pltpu.VMEM(key_cache.shape, key_cache.dtype),
                pltpu.VMEM(value_cache.shape, value_cache.dtype),
                pltpu.VMEM(summary_keys.shape, summary_keys.dtype),
                pltpu.VMEM(summary_values.shape, summary_values.dtype),
                pltpu.SMEM(owner_map.shape, owner_map.dtype),
                pltpu.VMEM(super_ids.shape, super_ids.dtype),
                pltpu.VMEM(fine_ids.shape, fine_ids.dtype),
                pltpu.VMEM((seq_size, groups, per_source, head_dim), jnp.bfloat16),
                pltpu.VMEM((requests, 2 * heads, head_dim), jnp.bfloat16),
                pltpu.VMEM((devices, out_rows, 2 * heads, head_dim), jnp.bfloat16),
                pltpu.SemaphoreType.DMA((6,)),
                pltpu.SemaphoreType.DMA((2, groups)),
                pltpu.SemaphoreType.DMA,
                pltpu.SemaphoreType.DMA,
                pltpu.SemaphoreType.DMA,
                pltpu.SemaphoreType.DMA,
            ],
            compiler_params=pltpu.CompilerParams(collective_id=0, has_side_effects=True),
        )(queries, key_cache, value_cache, summary_keys, summary_values, owner_map, super_ids, fine_ids)

    in_specs = (
        P("seq", "rep", None),
        P("rep", "seq", None),
        P("rep", "seq", None),
        P("rep", "seq", None),
        P("rep", "seq", None),
        P(),
        P(None, "rep", None),
        P(None, "rep", None),
    )
    out_specs = P(("seq", "rep"), None, None)
    return jax.shard_map(shards, mesh=mesh, in_specs=in_specs, out_specs=out_specs, check_vma=False)
```

```python
import functools
import math

import jax
import jax.numpy as jnp
from jax import lax
from jax.experimental import pallas as pl
from jax.experimental.pallas import tpu as pltpu
from jax.sharding import PartitionSpec as P

BLK = 128
SUPER = 16
NEGATIVE = -1e30
LOG2E = math.log2(math.e)
CHUNK = 32
WIDTH = 16
UNROLL_LIMIT = 64


def repeat(count, body):
    if count <= UNROLL_LIMIT:
        for step in range(count):
            body(step)
    else:

        def rolled(step, carry):
            body(step)
            return carry

        lax.fori_loop(0, count, rolled, 0)


def kernel(
    seq_size,
    rep_size,
    q_hbm,
    k_hbm,
    v_hbm,
    sk_hbm,
    sv_hbm,
    owner_hbm,
    super_hbm,
    fine_hbm,
    out_ref,
    k_ref,
    v_ref,
    sk_ref,
    sv_ref,
    owner_ref,
    super_ref,
    fine_ref,
    q_all,
    part_values,
    part_stats,
    landed_values,
    landed_stats,
    in_sems,
    kv_sems,
    q_send,
    q_recv,
    p_send,
    p_recv,
):
    my_seq = lax.axis_index("seq")
    my_rep = lax.axis_index("rep")
    devices = seq_size * rep_size
    own_rows, heads, head_dim = q_hbm.shape
    groups, tokens = k_ref.shape[:2]
    per_group = heads // groups
    slot_count = owner_ref.shape[0]
    out_rows = out_ref.shape[0]
    blocks = tokens // BLK
    near = q_recv.shape[0]
    sources = seq_size // near
    width = sources * own_rows
    my_block = lax.div(my_seq, sources)
    my_place = lax.rem(my_seq, sources)

    barrier = pltpu.get_barrier_semaphore()

    def reach(seq, rep):
        return dict(device_id=(seq, rep), device_id_type=pl.DeviceIdType.MESH)

    def greet_seq(step):
        pl.semaphore_signal(barrier, inc=1, **reach(lax.rem(my_seq + step + 1, seq_size), my_rep))

    def greet_rep(step):
        pl.semaphore_signal(barrier, inc=1, **reach(my_seq, lax.rem(my_rep + step + 1, rep_size)))

    repeat(seq_size - 1, greet_seq)
    repeat(rep_size - 1, greet_rep)

    mine = q_all.at[pl.ds(my_seq * own_rows, own_rows)]
    small = [
        pltpu.make_async_copy(src, dst, in_sems.at[i])
        for i, (src, dst) in enumerate(
            (
                (q_hbm, mine),
                (owner_hbm, owner_ref),
                (super_hbm, super_ref),
                (fine_hbm, fine_ref),
                (sk_hbm, sk_ref),
                (sv_hbm, sv_ref),
            )
        )
    ]
    for copy in small:
        copy.start()
    big = []
    for g in range(groups):
        big.append(pltpu.make_async_copy(k_hbm.at[g], k_ref.at[g], kv_sems.at[0, g]))
        big.append(pltpu.make_async_copy(v_hbm.at[g], v_ref.at[g], kv_sems.at[1, g]))
    for copy in big:
        copy.start()

    pl.semaphore_wait(barrier, seq_size - 1 + rep_size - 1)

    def send_query(away, place):
        block = lax.rem(my_block + away, near)
        pltpu.make_async_remote_copy(
            src_ref=q_hbm,
            dst_ref=mine,
            send_sem=q_send,
            recv_sem=q_recv.at[(near - away) % near],
            **reach(block * sources + place, my_rep),
        ).start()

    def send_block(step):
        away = near - 1 - step
        for place in range(sources):
            send_query(away, lax.rem(my_place + place, sources))

    repeat(near - 1, send_block)
    for place in range(1, sources):
        send_query(0, lax.rem(my_place + place, sources))

    for copy in small:
        copy.wait()

    if slot_count <= UNROLL_LIMIT:
        here = jnp.int32(0)
        for j in range(slot_count):
            here = here + jnp.where(owner_ref[j] == my_seq, j, 0)
    else:
        here = lax.fori_loop(
            0, slot_count, lambda j, total: total + jnp.where(owner_ref[j] == my_seq, j, 0), jnp.int32(0)
        )
    here = here.astype(jnp.float32)

    rows = width * per_group
    pairs = width // 2
    row_of = lax.broadcasted_iota(jnp.int32, (rows, CHUNK), 0)
    lane_of = lax.broadcasted_iota(jnp.int32, (rows, CHUNK), 1)
    scaling = head_dim ** (-0.5) * LOG2E
    sub = lax.broadcasted_iota(jnp.int32, (pairs, heads, head_dim), 1)
    lane = lax.broadcasted_iota(jnp.int32, (pairs, heads, head_dim), 2)
    top = sub < per_group
    diagonal = sub == lane

    def selection(first, g):
        chunk = lax.div(first, CHUNK)
        low = (lane_of - lax.rem(first, CHUNK)) * per_group
        expand = jnp.where((row_of >= low) & (row_of < low + per_group), 1.0, 0.0).astype(jnp.bfloat16)
        fine = fine_ref[chunk, g].astype(jnp.float32).astype(jnp.bfloat16)
        supers = super_ref[chunk, g].astype(jnp.float32).astype(jnp.bfloat16)
        contract = (((1,), (1,)), ((), ()))
        fine = lax.dot_general(expand, fine, contract, preferred_element_type=jnp.float32)
        supers = lax.dot_general(expand, supers, contract, preferred_element_type=jnp.float32)
        place = lax.broadcasted_iota(jnp.int32, supers.shape, 1).astype(jnp.float32) + 1.0
        place = jnp.sum(jnp.where(supers == here, place, 0.0), axis=1, keepdims=True)
        at = (fine - SUPER * (place - 1.0)).astype(jnp.int32)
        valid = (at >= 0) & (at < SUPER) & (place > 0.0)
        bit = jnp.left_shift(1, jnp.clip(at, 0, SUPER - 1)).astype(jnp.float32)
        bits = jnp.sum(jnp.where(valid, bit, 0.0), axis=1, keepdims=True).astype(jnp.int32)
        return place, bits

    def regroup(a, b):
        return jnp.where(top, a, pltpu.roll(b, per_group, 1)), jnp.where(top, pltpu.roll(a, per_group, 1), b)

    def attend(query, g, place, bits):
        bits = jnp.broadcast_to(bits, (rows, BLK))
        scores = lax.dot_general(
            query.astype(jnp.bfloat16), k_ref[g], (((1,), (1,)), ((), ())), preferred_element_type=jnp.float32
        )
        masked = []
        for b in range(blocks):
            one = scores[:, b * BLK : (b + 1) * BLK]
            masked.append(jnp.where((bits & (1 << b)) != 0, one, NEGATIVE))
        peak = functools.reduce(jnp.maximum, masked)
        peak = jnp.max(peak, axis=1, keepdims=True)
        weights = [jnp.exp2((one - peak) * scaling) for one in masked]
        total = jnp.sum(functools.reduce(jnp.add, weights), axis=1, keepdims=True)
        packed = jnp.concatenate([one.astype(jnp.bfloat16) for one in weights], axis=1)
        summed = jnp.dot(packed, v_ref[g], preferred_element_type=jnp.float32)
        coarse = jnp.sum(query * sk_ref[:, g].astype(jnp.float32), axis=1, keepdims=True)
        coarse = coarse * scaling + math.log2(SUPER)
        stat = jnp.where(place > 0.0, peak * scaling + jnp.log2(total), coarse)
        value = jnp.where(place > 0.0, summed / total, sv_ref[:, g].astype(jnp.float32))
        stat = jnp.broadcast_to(stat, (rows, head_dim))
        return value.reshape(pairs, heads, head_dim), stat.reshape(pairs, heads, head_dim)

    def block_parts(first, chosen):
        raw = q_all[pl.ds(first, width)].astype(jnp.float32).reshape(pairs, 2, heads, head_dim)
        queries = [one.reshape(rows, head_dim) for one in regroup(raw[:, 0], raw[:, 1])]
        (value_a, stat_a), (value_b, stat_b) = [attend(queries[g], g, *chosen[g]) for g in range(groups)]
        values = [one.astype(jnp.bfloat16) for one in regroup(value_a, value_b)]
        stats = [
            jnp.sum(jnp.where(diagonal, one, 0.0), axis=1, keepdims=True) for one in regroup(stat_a, stat_b)
        ]
        for which in range(2):
            for pair in range(pairs):
                part_values[first + 2 * pair + which] = values[which][pair]
                part_stats[first + 2 * pair + which] = stats[which][pair]

    slot = pl.ds(my_rep * seq_size + my_seq, 1)
    messages = ((part_values, landed_values), (part_stats, landed_stats))

    def send_parts(first, start, skip):
        targets = width // out_rows
        for step in range(skip, targets):
            target = lax.rem(start + step, targets)
            there = lax.div(first, out_rows) + target
            for kind, (source, landed) in enumerate(messages):
                pltpu.make_async_remote_copy(
                    src_ref=source.at[pl.ds(first + target * out_rows, out_rows)],
                    dst_ref=landed.at[my_rep * seq_size + my_seq],
                    send_sem=p_send.at[kind],
                    recv_sem=p_recv.at[kind],
                    **reach(lax.div(there, rep_size), lax.rem(there, rep_size)),
                ).start()

    def wait_block(away, count):
        got = q_all.at[pl.ds(0, count * own_rows)]
        pltpu.make_async_copy(got, got, q_recv.at[away]).wait()

    def block_first(away):
        return lax.rem(my_block + away, near) * width

    mine_at = my_place * rep_size + my_rep

    def run_block(away, chosen):
        wait_block(away, sources)
        block_parts(block_first(away), chosen)
        send_parts(block_first(away), mine_at, 0)

    def choose(away):
        return [selection(block_first(away), g) for g in range(groups)]

    ahead = [choose(away) for away in range(near)] if near <= 2 else None
    for copy in big:
        copy.wait()
    if sources > 1:
        wait_block(0, sources - 1)
    block_parts(block_first(0), ahead[0] if ahead else choose(0))
    send_parts(block_first(0), mine_at, 1)
    own = block_first(0) + mine_at * out_rows
    landed_values[slot] = part_values[pl.ds(own, out_rows)][None]
    landed_stats[slot] = part_stats[pl.ds(own, out_rows)][None]

    if ahead:
        for away in range(1, near):
            run_block(away, ahead[away])
    else:

        def block_step(away, carry):
            run_block(away, choose(away))
            return carry

        lax.fori_loop(1, near, block_step, 0)

    for kind, (_, landed) in enumerate(messages):
        got = landed.at[pl.ds(0, devices - 1)]
        pltpu.make_async_copy(got, got, p_recv.at[kind]).wait()

    same = lax.broadcasted_iota(jnp.int32, (heads, head_dim), 0) == lax.broadcasted_iota(
        jnp.int32, (heads, head_dim), 1
    )
    for i in range(out_rows):
        for p in range(rep_size):
            stats = [landed_stats[p * seq_size + s, i] for s in range(seq_size)]
            peak = functools.reduce(jnp.maximum, stats)
            factors = [jnp.exp2(stat - peak) for stat in stats]
            total = functools.reduce(jnp.add, factors)
            summed = jnp.zeros((heads, head_dim), jnp.float32)
            for s in range(seq_size):
                share = jnp.where(same, factors[s] / total, 0.0)
                share = jnp.sum(share, axis=1, keepdims=True)
                summed = summed + share * landed_values[p * seq_size + s, i].astype(jnp.float32)
            out_ref[i, p * heads : (p + 1) * heads] = summed.astype(out_ref.dtype)

    sent = q_all.at[pl.ds(0, (seq_size - 1) * own_rows)]
    pltpu.make_async_copy(sent, sent, q_send).wait()
    for kind, (_, landed) in enumerate(messages):
        sent = landed.at[pl.ds(0, devices - 1)]
        pltpu.make_async_copy(sent, sent, p_send.at[kind]).wait()


def solution(mesh):
    seq_size = mesh.shape["seq"]
    rep_size = mesh.shape["rep"]

    def shards(queries, key_cache, value_cache, summary_keys, summary_values, owner_map, super_ids, fine_ids):
        own_rows, heads, head_dim = queries.shape
        groups, tokens = key_cache.shape[:2]
        requests = super_ids.shape[0]
        devices = seq_size * rep_size
        out_rows = own_rows // rep_size
        sources = math.gcd(seq_size, max(WIDTH // own_rows, 1))
        assert summary_keys.shape[1] == 1 and tokens == SUPER * BLK
        assert groups == 2 and heads == 8 and own_rows % rep_size == 0 and own_rows % 2 == 0
        assert requests % CHUNK == 0 and CHUNK % (sources * own_rows) == 0
        hbm = pl.BlockSpec(memory_space=pltpu.HBM)
        summary_keys = jnp.transpose(summary_keys, (1, 0, 2))
        summary_values = jnp.transpose(summary_values, (1, 0, 2))
        chunked = (requests // CHUNK, CHUNK, groups, -1)
        super_ids = jnp.transpose(super_ids.reshape(chunked), (0, 2, 3, 1))
        fine_ids = jnp.transpose(fine_ids.reshape(chunked), (0, 2, 3, 1))
        return pl.pallas_call(
            functools.partial(kernel, seq_size, rep_size),
            out_shape=pltpu.VMEM((out_rows, rep_size * heads, head_dim), jnp.bfloat16),
            in_specs=[hbm] * 8,
            out_specs=pl.BlockSpec(memory_space=pltpu.VMEM),
            scratch_shapes=[
                pltpu.VMEM(key_cache.shape, key_cache.dtype),
                pltpu.VMEM(value_cache.shape, value_cache.dtype),
                pltpu.VMEM(summary_keys.shape, summary_keys.dtype),
                pltpu.VMEM(summary_values.shape, summary_values.dtype),
                pltpu.SMEM(owner_map.shape, owner_map.dtype),
                pltpu.VMEM(super_ids.shape, super_ids.dtype),
                pltpu.VMEM(fine_ids.shape, fine_ids.dtype),
                pltpu.VMEM((seq_size * own_rows, heads, head_dim), jnp.bfloat16),
                pltpu.VMEM((requests, heads, head_dim), jnp.bfloat16),
                pltpu.VMEM((requests, 1, head_dim), jnp.float32),
                pltpu.VMEM((devices, out_rows, heads, head_dim), jnp.bfloat16),
                pltpu.VMEM((devices, out_rows, 1, head_dim), jnp.float32),
                pltpu.SemaphoreType.DMA((6,)),
                pltpu.SemaphoreType.DMA((2, groups)),
                pltpu.SemaphoreType.DMA,
                pltpu.SemaphoreType.DMA((seq_size // sources,)),
                pltpu.SemaphoreType.DMA((2,)),
                pltpu.SemaphoreType.DMA((2,)),
            ],
            compiler_params=pltpu.CompilerParams(collective_id=0, has_side_effects=True),
        )(queries, key_cache, value_cache, summary_keys, summary_values, owner_map, super_ids, fine_ids)

    in_specs = (
        P("seq", "rep", None),
        P("rep", "seq", None),
        P("rep", "seq", None),
        P("rep", "seq", None),
        P("rep", "seq", None),
        P(),
        P(None, "rep", None),
        P(None, "rep", None),
    )
    out_specs = P(("seq", "rep"), None, None)
    return jax.shard_map(shards, mesh=mesh, in_specs=in_specs, out_specs=out_specs, check_vma=False)
```

```python
import functools
import math

import jax
import jax.numpy as jnp
from jax import lax
from jax.experimental import pallas as pl
from jax.experimental.pallas import tpu as pltpu
from jax.sharding import PartitionSpec as P

BLK = 128
SUPER = 16
NEGATIVE = -1e30
LOG2E = math.log2(math.e)
CHUNK = 32
NEAR = 4
UNROLL_LIMIT = 64


def repeat(count, body):
    if count <= UNROLL_LIMIT:
        for step in range(count):
            body(step)
    else:

        def rolled(step, carry):
            body(step)
            return carry

        lax.fori_loop(0, count, rolled, 0)


def kernel(
    seq_size,
    rep_size,
    q_hbm,
    k_hbm,
    v_hbm,
    sk_hbm,
    sv_hbm,
    owner_hbm,
    super_hbm,
    fine_hbm,
    out_ref,
    k_ref,
    v_ref,
    sk_ref,
    sv_ref,
    owner_ref,
    super_ref,
    fine_ref,
    q_all,
    part_values,
    part_stats,
    landed_values,
    landed_stats,
    in_sems,
    kv_sems,
    q_send,
    q_far,
    q_near,
    p_send,
    p_recv,
):
    my_seq = lax.axis_index("seq")
    my_rep = lax.axis_index("rep")
    devices = seq_size * rep_size
    own_rows, heads, head_dim = q_hbm.shape
    groups, tokens = k_ref.shape[:2]
    per_group = heads // groups
    slot_count = owner_ref.shape[0]
    out_rows = out_ref.shape[0]
    blocks = tokens // BLK
    near = q_far.shape[0]
    sources = seq_size // near
    width = CHUNK
    chunks = q_all.shape[0] // CHUNK
    my_block = lax.div(my_seq, sources)
    my_place = lax.rem(my_seq, sources)

    barrier = pltpu.get_barrier_semaphore()

    def reach(seq, rep):
        return dict(device_id=(seq, rep), device_id_type=pl.DeviceIdType.MESH)

    def same_block(step):
        return my_block * sources + lax.rem(my_place + step, sources)

    def same_place(step):
        return lax.rem(my_block + step, near) * sources + my_place

    def greet_near(step):
        pl.semaphore_signal(barrier, inc=1, **reach(same_block(step + 1), my_rep))

    def greet_far(step):
        pl.semaphore_signal(barrier, inc=1, **reach(same_place(step + 1), my_rep))

    def greet_rep(step):
        pl.semaphore_signal(barrier, inc=1, **reach(my_seq, lax.rem(my_rep + step + 1, rep_size)))

    repeat(near - 1, greet_far)
    repeat(sources - 1, greet_near)
    repeat(rep_size - 1, greet_rep)

    mine = q_all.at[pl.ds(my_seq * own_rows, own_rows)]
    small = [
        pltpu.make_async_copy(src, dst, in_sems.at[i])
        for i, (src, dst) in enumerate(
            (
                (q_hbm, mine),
                (owner_hbm, owner_ref),
                (super_hbm, super_ref),
                (fine_hbm, fine_ref),
                (sk_hbm, sk_ref),
                (sv_hbm, sv_ref),
            )
        )
    ]
    for copy in small:
        copy.start()
    big = []
    for g in range(groups):
        big.append(pltpu.make_async_copy(k_hbm.at[g], k_ref.at[g], kv_sems.at[0, g]))
        big.append(pltpu.make_async_copy(v_hbm.at[g], v_ref.at[g], kv_sems.at[1, g]))
    for copy in big:
        copy.start()

    pl.semaphore_wait(barrier, near - 1 + sources - 1 + rep_size - 1)

    def send_far(step):
        pltpu.make_async_remote_copy(
            src_ref=q_hbm,
            dst_ref=mine,
            send_sem=q_send.at[0],
            recv_sem=q_far.at[(near - 1 - step) % near],
            **reach(same_place(step + 1), my_rep),
        ).start()

    repeat(near - 1, send_far)
    for step in range(1, sources):
        pltpu.make_async_remote_copy(
            src_ref=q_hbm,
            dst_ref=mine,
            send_sem=q_send.at[0],
            recv_sem=q_near,
            **reach(same_block(step), my_rep),
        ).start()

    for copy in small[1:]:
        copy.wait()

    if slot_count <= UNROLL_LIMIT:
        here = jnp.int32(0)
        for j in range(slot_count):
            here = here + jnp.where(owner_ref[j] == my_seq, j, 0)
    else:
        here = lax.fori_loop(
            0, slot_count, lambda j, total: total + jnp.where(owner_ref[j] == my_seq, j, 0), jnp.int32(0)
        )
    here = here.astype(jnp.float32)

    rows = width * per_group
    pairs = width // 2
    row_of = lax.broadcasted_iota(jnp.int32, (rows, CHUNK), 0)
    lane_of = lax.broadcasted_iota(jnp.int32, (rows, CHUNK), 1)
    scaling = head_dim ** (-0.5) * LOG2E
    sub = lax.broadcasted_iota(jnp.int32, (pairs, heads, head_dim), 1)
    lane = lax.broadcasted_iota(jnp.int32, (pairs, heads, head_dim), 2)
    top = sub < per_group
    diagonal = sub == lane

    def selection(first, g):
        chunk = lax.div(first, CHUNK)
        low = (lane_of - lax.rem(first, CHUNK)) * per_group
        expand = jnp.where((row_of >= low) & (row_of < low + per_group), 1.0, 0.0).astype(jnp.bfloat16)
        fine = fine_ref[chunk, g].astype(jnp.float32).astype(jnp.bfloat16)
        supers = super_ref[chunk, g].astype(jnp.float32).astype(jnp.bfloat16)
        contract = (((1,), (1,)), ((), ()))
        fine = lax.dot_general(expand, fine, contract, preferred_element_type=jnp.float32)
        supers = lax.dot_general(expand, supers, contract, preferred_element_type=jnp.float32)
        place = lax.broadcasted_iota(jnp.int32, supers.shape, 1).astype(jnp.float32) + 1.0
        place = jnp.sum(jnp.where(supers == here, place, 0.0), axis=1, keepdims=True)
        at = (fine - SUPER * (place - 1.0)).astype(jnp.int32)
        valid = (at >= 0) & (at < SUPER) & (place > 0.0)
        bit = jnp.left_shift(1, jnp.clip(at, 0, SUPER - 1)).astype(jnp.float32)
        bits = jnp.sum(jnp.where(valid, bit, 0.0), axis=1, keepdims=True).astype(jnp.int32)
        return place, bits

    def regroup(a, b):
        return jnp.where(top, a, pltpu.roll(b, per_group, 1)), jnp.where(top, pltpu.roll(a, per_group, 1), b)

    def attend(query, g, place, bits):
        bits = jnp.broadcast_to(bits, (rows, BLK))
        scores = lax.dot_general(
            query.astype(jnp.bfloat16), k_ref[g], (((1,), (1,)), ((), ())), preferred_element_type=jnp.float32
        )
        masked = []
        for b in range(blocks):
            one = scores[:, b * BLK : (b + 1) * BLK]
            masked.append(jnp.where((bits & (1 << b)) != 0, one, NEGATIVE))
        peak = functools.reduce(jnp.maximum, masked)
        peak = jnp.max(peak, axis=1, keepdims=True)
        weights = [jnp.exp2((one - peak) * scaling) for one in masked]
        total = jnp.sum(functools.reduce(jnp.add, weights), axis=1, keepdims=True)
        packed = jnp.concatenate([one.astype(jnp.bfloat16) for one in weights], axis=1)
        summed = jnp.dot(packed, v_ref[g], preferred_element_type=jnp.float32)
        coarse = jnp.sum(query * sk_ref[:, g].astype(jnp.float32), axis=1, keepdims=True)
        coarse = coarse * scaling + math.log2(SUPER)
        stat = jnp.where(place > 0.0, peak * scaling + jnp.log2(total), coarse)
        value = jnp.where(place > 0.0, summed / total, sv_ref[:, g].astype(jnp.float32))
        stat = jnp.broadcast_to(stat, (rows, head_dim))
        return value.reshape(pairs, heads, head_dim), stat.reshape(pairs, heads, head_dim)

    def block_parts(first, chosen):
        raw = q_all[pl.ds(first, width)].astype(jnp.float32).reshape(pairs, 2, heads, head_dim)
        queries = [one.reshape(rows, head_dim) for one in regroup(raw[:, 0], raw[:, 1])]
        (value_a, stat_a), (value_b, stat_b) = [attend(queries[g], g, *chosen[g]) for g in range(groups)]
        values = [one.astype(jnp.bfloat16) for one in regroup(value_a, value_b)]
        stats = [
            jnp.sum(jnp.where(diagonal, one, 0.0), axis=1, keepdims=True) for one in regroup(stat_a, stat_b)
        ]
        for which in range(2):
            for pair in range(pairs):
                part_values[first + 2 * pair + which] = values[which][pair]
                part_stats[first + 2 * pair + which] = stats[which][pair]

    slot = pl.ds(my_rep * seq_size + my_seq, 1)
    messages = ((part_values, landed_values), (part_stats, landed_stats))

    def send_parts(first, start, skip):
        targets = width // out_rows
        for step in range(skip, targets):
            target = lax.rem(start + step, targets)
            there = lax.div(first, out_rows) + target
            for kind, (source, landed) in enumerate(messages):
                pltpu.make_async_remote_copy(
                    src_ref=source.at[pl.ds(first + target * out_rows, out_rows)],
                    dst_ref=landed.at[my_rep * seq_size + my_seq],
                    send_sem=p_send.at[kind],
                    recv_sem=p_recv.at[kind],
                    **reach(lax.div(there, rep_size), lax.rem(there, rep_size)),
                ).start()

    def choose(first):
        return [selection(first, g) for g in range(groups)]

    my_chunk = lax.div(my_seq * own_rows, CHUNK)
    ahead = choose(my_chunk * CHUNK)

    def forward(step):
        held = q_all.at[pl.ds(same_place(step + 1) * own_rows, own_rows)]
        pltpu.make_async_copy(held, held, q_far.at[step + 1]).wait()
        for place in range(1, sources):
            pltpu.make_async_remote_copy(
                src_ref=held,
                dst_ref=held,
                send_sem=q_send.at[1],
                recv_sem=q_near,
                **reach(same_block(place), my_rep),
            ).start()

    repeat(near - 1, forward)
    small[0].wait()
    for copy in big:
        copy.wait()
    passed = (sources - 1) * near * own_rows
    if sources > 1:
        got = q_all.at[pl.ds(0, passed)]
        pltpu.make_async_copy(got, got, q_near).wait()

    own = (my_seq * rep_size + my_rep) * out_rows
    mine_at = lax.rem(my_seq * own_rows, CHUNK) // out_rows + my_rep
    block_parts(my_chunk * CHUNK, ahead)
    send_parts(my_chunk * CHUNK, mine_at, 1)
    landed_values[slot] = part_values[pl.ds(own, out_rows)][None]
    landed_stats[slot] = part_stats[pl.ds(own, out_rows)][None]

    if chunks > 1:

        def chunk_step(step, carry):
            first = lax.rem(my_chunk + step, chunks) * CHUNK
            block_parts(first, choose(first))
            send_parts(first, mine_at, 0)
            return carry

        lax.fori_loop(1, chunks, chunk_step, 0)

    for kind, (_, landed) in enumerate(messages):
        got = landed.at[pl.ds(0, devices - 1)]
        pltpu.make_async_copy(got, got, p_recv.at[kind]).wait()

    same = lax.broadcasted_iota(jnp.int32, (heads, head_dim), 0) == lax.broadcasted_iota(
        jnp.int32, (heads, head_dim), 1
    )
    for i in range(out_rows):
        for p in range(rep_size):
            stats = [landed_stats[p * seq_size + s, i] for s in range(seq_size)]
            peak = functools.reduce(jnp.maximum, stats)
            factors = [jnp.exp2(stat - peak) for stat in stats]
            total = functools.reduce(jnp.add, factors)
            summed = jnp.zeros((heads, head_dim), jnp.float32)
            for s in range(seq_size):
                share = jnp.where(same, factors[s] / total, 0.0)
                share = jnp.sum(share, axis=1, keepdims=True)
                summed = summed + share * landed_values[p * seq_size + s, i].astype(jnp.float32)
            out_ref[i, p * heads : (p + 1) * heads] = summed.astype(out_ref.dtype)

    for i, count in enumerate((near - 1 + sources - 1, (near - 1) * (sources - 1))):
        if count > 0:
            sent = q_all.at[pl.ds(0, count * own_rows)]
            pltpu.make_async_copy(sent, sent, q_send.at[i]).wait()
    for kind, (_, landed) in enumerate(messages):
        sent = landed.at[pl.ds(0, devices - 1)]
        pltpu.make_async_copy(sent, sent, p_send.at[kind]).wait()


def solution(mesh):
    seq_size = mesh.shape["seq"]
    rep_size = mesh.shape["rep"]

    def shards(queries, key_cache, value_cache, summary_keys, summary_values, owner_map, super_ids, fine_ids):
        own_rows, heads, head_dim = queries.shape
        groups, tokens = key_cache.shape[:2]
        requests = super_ids.shape[0]
        devices = seq_size * rep_size
        out_rows = own_rows // rep_size
        sources = math.gcd(seq_size, NEAR)
        assert summary_keys.shape[1] == 1 and tokens == SUPER * BLK
        assert groups == 2 and heads == 8 and own_rows % rep_size == 0 and own_rows % 2 == 0
        assert requests % CHUNK == 0 and CHUNK % own_rows == 0
        hbm = pl.BlockSpec(memory_space=pltpu.HBM)
        summary_keys = jnp.transpose(summary_keys, (1, 0, 2))
        summary_values = jnp.transpose(summary_values, (1, 0, 2))
        chunked = (requests // CHUNK, CHUNK, groups, -1)
        super_ids = jnp.transpose(super_ids.reshape(chunked), (0, 2, 3, 1))
        fine_ids = jnp.transpose(fine_ids.reshape(chunked), (0, 2, 3, 1))
        return pl.pallas_call(
            functools.partial(kernel, seq_size, rep_size),
            out_shape=pltpu.VMEM((out_rows, rep_size * heads, head_dim), jnp.bfloat16),
            in_specs=[hbm] * 8,
            out_specs=pl.BlockSpec(memory_space=pltpu.VMEM),
            scratch_shapes=[
                pltpu.VMEM(key_cache.shape, key_cache.dtype),
                pltpu.VMEM(value_cache.shape, value_cache.dtype),
                pltpu.VMEM(summary_keys.shape, summary_keys.dtype),
                pltpu.VMEM(summary_values.shape, summary_values.dtype),
                pltpu.SMEM(owner_map.shape, owner_map.dtype),
                pltpu.VMEM(super_ids.shape, super_ids.dtype),
                pltpu.VMEM(fine_ids.shape, fine_ids.dtype),
                pltpu.VMEM((seq_size * own_rows, heads, head_dim), jnp.bfloat16),
                pltpu.VMEM((requests, heads, head_dim), jnp.bfloat16),
                pltpu.VMEM((requests, 1, head_dim), jnp.float32),
                pltpu.VMEM((devices, out_rows, heads, head_dim), jnp.bfloat16),
                pltpu.VMEM((devices, out_rows, 1, head_dim), jnp.float32),
                pltpu.SemaphoreType.DMA((6,)),
                pltpu.SemaphoreType.DMA((2, groups)),
                pltpu.SemaphoreType.DMA((2,)),
                pltpu.SemaphoreType.DMA((seq_size // sources,)),
                pltpu.SemaphoreType.DMA,
                pltpu.SemaphoreType.DMA((2,)),
                pltpu.SemaphoreType.DMA((2,)),
            ],
            compiler_params=pltpu.CompilerParams(collective_id=0, has_side_effects=True),
        )(queries, key_cache, value_cache, summary_keys, summary_values, owner_map, super_ids, fine_ids)

    in_specs = (
        P("seq", "rep", None),
        P("rep", "seq", None),
        P("rep", "seq", None),
        P("rep", "seq", None),
        P("rep", "seq", None),
        P(),
        P(None, "rep", None),
        P(None, "rep", None),
    )
    out_specs = P(("seq", "rep"), None, None)
    return jax.shard_map(shards, mesh=mesh, in_specs=in_specs, out_specs=out_specs, check_vma=False)
```

```python
import functools
import math

import jax
import jax.numpy as jnp
from jax import lax
from jax.experimental import pallas as pl
from jax.experimental.pallas import tpu as pltpu
from jax.sharding import PartitionSpec as P

BLK = 128
SUPER = 16
NEGATIVE = -1e30
LOG2E = math.log2(math.e)
CHUNK = 32
WIDTH = 32
UNROLL_LIMIT = 64


def repeat(count, body):
    if count <= UNROLL_LIMIT:
        for step in range(count):
            body(step)
    else:

        def rolled(step, carry):
            body(step)
            return carry

        lax.fori_loop(0, count, rolled, 0)


def kernel(
    seq_size,
    rep_size,
    q_hbm,
    k_hbm,
    v_hbm,
    sk_hbm,
    sv_hbm,
    owner_hbm,
    super_hbm,
    fine_hbm,
    out_ref,
    k_ref,
    v_ref,
    sk_ref,
    sv_ref,
    owner_ref,
    super_ref,
    fine_ref,
    q_all,
    part_values,
    part_stats,
    landed_values,
    landed_stats,
    in_sems,
    kv_sems,
    q_send,
    q_recv,
    p_send,
    p_recv,
):
    my_seq = lax.axis_index("seq")
    my_rep = lax.axis_index("rep")
    devices = seq_size * rep_size
    own_rows, heads, head_dim = q_hbm.shape
    groups, tokens = k_ref.shape[:2]
    per_group = heads // groups
    slot_count = owner_ref.shape[0]
    out_rows = out_ref.shape[0]
    blocks = tokens // BLK
    near = q_recv.shape[0]
    sources = seq_size // near
    width = sources * own_rows
    my_block = lax.div(my_seq, sources)
    my_place = lax.rem(my_seq, sources)

    barrier = pltpu.get_barrier_semaphore()

    def reach(seq, rep):
        return dict(device_id=(seq, rep), device_id_type=pl.DeviceIdType.MESH)

    def greet_seq(step):
        pl.semaphore_signal(barrier, inc=1, **reach(lax.rem(my_seq + step + 1, seq_size), my_rep))

    def greet_rep(step):
        pl.semaphore_signal(barrier, inc=1, **reach(my_seq, lax.rem(my_rep + step + 1, rep_size)))

    repeat(seq_size - 1, greet_seq)
    repeat(rep_size - 1, greet_rep)

    mine = q_all.at[pl.ds(my_seq * own_rows, own_rows)]
    small = [
        pltpu.make_async_copy(src, dst, in_sems.at[i])
        for i, (src, dst) in enumerate(
            (
                (q_hbm, mine),
                (owner_hbm, owner_ref),
                (super_hbm, super_ref),
                (fine_hbm, fine_ref),
                (sk_hbm, sk_ref),
                (sv_hbm, sv_ref),
            )
        )
    ]
    for copy in small:
        copy.start()
    big = []
    for g in range(groups):
        big.append(pltpu.make_async_copy(k_hbm.at[g], k_ref.at[g], kv_sems.at[0, g]))
        big.append(pltpu.make_async_copy(v_hbm.at[g], v_ref.at[g], kv_sems.at[1, g]))
    for copy in big:
        copy.start()

    pl.semaphore_wait(barrier, seq_size - 1 + rep_size - 1)

    def send_query(away, place):
        block = lax.rem(my_block + away, near)
        pltpu.make_async_remote_copy(
            src_ref=q_hbm,
            dst_ref=mine,
            send_sem=q_send,
            recv_sem=q_recv.at[(near - away) % near],
            **reach(block * sources + place, my_rep),
        ).start()

    def send_block(step):
        away = near - 1 - step
        for place in range(sources):
            send_query(away, lax.rem(my_place + place, sources))

    repeat(near - 1, send_block)
    for place in range(1, sources):
        send_query(0, lax.rem(my_place + place, sources))

    for copy in small:
        copy.wait()

    if slot_count <= UNROLL_LIMIT:
        here = jnp.int32(0)
        for j in range(slot_count):
            here = here + jnp.where(owner_ref[j] == my_seq, j, 0)
    else:
        here = lax.fori_loop(
            0, slot_count, lambda j, total: total + jnp.where(owner_ref[j] == my_seq, j, 0), jnp.int32(0)
        )
    here = here.astype(jnp.float32)

    rows = width * per_group
    pairs = width // 2
    row_of = lax.broadcasted_iota(jnp.int32, (rows, CHUNK), 0)
    lane_of = lax.broadcasted_iota(jnp.int32, (rows, CHUNK), 1)
    scaling = head_dim ** (-0.5) * LOG2E
    sub = lax.broadcasted_iota(jnp.int32, (pairs, heads, head_dim), 1)
    lane = lax.broadcasted_iota(jnp.int32, (pairs, heads, head_dim), 2)
    top = sub < per_group
    diagonal = sub == lane

    def selection(first, g):
        chunk = lax.div(first, CHUNK)
        low = (lane_of - lax.rem(first, CHUNK)) * per_group
        expand = jnp.where((row_of >= low) & (row_of < low + per_group), 1.0, 0.0).astype(jnp.bfloat16)
        fine = fine_ref[chunk, g].astype(jnp.float32).astype(jnp.bfloat16)
        supers = super_ref[chunk, g].astype(jnp.float32).astype(jnp.bfloat16)
        contract = (((1,), (1,)), ((), ()))
        fine = lax.dot_general(expand, fine, contract, preferred_element_type=jnp.float32)
        supers = lax.dot_general(expand, supers, contract, preferred_element_type=jnp.float32)
        place = lax.broadcasted_iota(jnp.int32, supers.shape, 1).astype(jnp.float32) + 1.0
        place = jnp.sum(jnp.where(supers == here, place, 0.0), axis=1, keepdims=True)
        at = (fine - SUPER * (place - 1.0)).astype(jnp.int32)
        valid = (at >= 0) & (at < SUPER) & (place > 0.0)
        bit = jnp.left_shift(1, jnp.clip(at, 0, SUPER - 1)).astype(jnp.float32)
        bits = jnp.sum(jnp.where(valid, bit, 0.0), axis=1, keepdims=True).astype(jnp.int32)
        return place, bits

    def regroup(a, b):
        return jnp.where(top, a, pltpu.roll(b, per_group, 1)), jnp.where(top, pltpu.roll(a, per_group, 1), b)

    def attend(query, g, place, bits):
        bits = jnp.broadcast_to(bits, (rows, BLK))
        scores = lax.dot_general(
            query.astype(jnp.bfloat16), k_ref[g], (((1,), (1,)), ((), ())), preferred_element_type=jnp.float32
        )
        masked = []
        for b in range(blocks):
            one = scores[:, b * BLK : (b + 1) * BLK]
            masked.append(jnp.where((bits & (1 << b)) != 0, one, NEGATIVE))
        peak = functools.reduce(jnp.maximum, masked)
        peak = jnp.max(peak, axis=1, keepdims=True)
        weights = [jnp.exp2((one - peak) * scaling) for one in masked]
        total = jnp.sum(functools.reduce(jnp.add, weights), axis=1, keepdims=True)
        packed = jnp.concatenate([one.astype(jnp.bfloat16) for one in weights], axis=1)
        summed = jnp.dot(packed, v_ref[g], preferred_element_type=jnp.float32)
        coarse = jnp.sum(query * sk_ref[:, g].astype(jnp.float32), axis=1, keepdims=True)
        coarse = coarse * scaling + math.log2(SUPER)
        stat = jnp.where(place > 0.0, peak * scaling + jnp.log2(total), coarse)
        value = jnp.where(place > 0.0, summed / total, sv_ref[:, g].astype(jnp.float32))
        stat = jnp.broadcast_to(stat, (rows, head_dim))
        return value.reshape(pairs, heads, head_dim), stat.reshape(pairs, heads, head_dim)

    def block_parts(first, chosen):
        raw = q_all[pl.ds(first, width)].astype(jnp.float32).reshape(pairs, 2, heads, head_dim)
        queries = [one.reshape(rows, head_dim) for one in regroup(raw[:, 0], raw[:, 1])]
        (value_a, stat_a), (value_b, stat_b) = [attend(queries[g], g, *chosen[g]) for g in range(groups)]
        values = [one.astype(jnp.bfloat16) for one in regroup(value_a, value_b)]
        stats = [
            jnp.sum(jnp.where(diagonal, one, 0.0), axis=1, keepdims=True) for one in regroup(stat_a, stat_b)
        ]
        for which in range(2):
            for pair in range(pairs):
                part_values[first + 2 * pair + which] = values[which][pair]
                part_stats[first + 2 * pair + which] = stats[which][pair]

    slot = pl.ds(my_rep * seq_size + my_seq, 1)
    messages = ((part_values, landed_values), (part_stats, landed_stats))

    def send_parts(first, start, skip):
        targets = width // out_rows
        for step in range(skip, targets):
            target = lax.rem(start + step, targets)
            there = lax.div(first, out_rows) + target
            for kind, (source, landed) in enumerate(messages):
                pltpu.make_async_remote_copy(
                    src_ref=source.at[pl.ds(first + target * out_rows, out_rows)],
                    dst_ref=landed.at[my_rep * seq_size + my_seq],
                    send_sem=p_send.at[kind],
                    recv_sem=p_recv.at[kind],
                    **reach(lax.div(there, rep_size), lax.rem(there, rep_size)),
                ).start()

    def wait_block(away, count):
        got = q_all.at[pl.ds(0, count * own_rows)]
        pltpu.make_async_copy(got, got, q_recv.at[away]).wait()

    def block_first(away):
        return lax.rem(my_block + away, near) * width

    mine_at = my_place * rep_size + my_rep

    def run_block(away, chosen):
        wait_block(away, sources)
        block_parts(block_first(away), chosen)
        send_parts(block_first(away), mine_at, 0)

    def choose(away):
        return [selection(block_first(away), g) for g in range(groups)]

    ahead = [choose(away) for away in range(near)] if near <= 2 else None
    for copy in big:
        copy.wait()
    if sources > 1:
        wait_block(0, sources - 1)
    block_parts(block_first(0), ahead[0] if ahead else choose(0))
    send_parts(block_first(0), mine_at, 1)
    own = block_first(0) + mine_at * out_rows
    landed_values[slot] = part_values[pl.ds(own, out_rows)][None]
    landed_stats[slot] = part_stats[pl.ds(own, out_rows)][None]

    if ahead:
        for away in range(1, near):
            run_block(away, ahead[away])
    else:

        def block_step(away, carry):
            run_block(away, choose(away))
            return carry

        lax.fori_loop(1, near, block_step, 0)

    for kind, (_, landed) in enumerate(messages):
        got = landed.at[pl.ds(0, devices - 1)]
        pltpu.make_async_copy(got, got, p_recv.at[kind]).wait()

    same = lax.broadcasted_iota(jnp.int32, (heads, head_dim), 0) == lax.broadcasted_iota(
        jnp.int32, (heads, head_dim), 1
    )
    for i in range(out_rows):
        for p in range(rep_size):
            stats = [landed_stats[p * seq_size + s, i] for s in range(seq_size)]
            peak = functools.reduce(jnp.maximum, stats)
            factors = [jnp.exp2(stat - peak) for stat in stats]
            total = functools.reduce(jnp.add, factors)
            summed = jnp.zeros((heads, head_dim), jnp.float32)
            for s in range(seq_size):
                share = jnp.where(same, factors[s] / total, 0.0)
                share = jnp.sum(share, axis=1, keepdims=True)
                summed = summed + share * landed_values[p * seq_size + s, i].astype(jnp.float32)
            out_ref[i, p * heads : (p + 1) * heads] = summed.astype(out_ref.dtype)

    sent = q_all.at[pl.ds(0, (seq_size - 1) * own_rows)]
    pltpu.make_async_copy(sent, sent, q_send).wait()
    for kind, (_, landed) in enumerate(messages):
        sent = landed.at[pl.ds(0, devices - 1)]
        pltpu.make_async_copy(sent, sent, p_send.at[kind]).wait()


def solution(mesh):
    seq_size = mesh.shape["seq"]
    rep_size = mesh.shape["rep"]

    def shards(queries, key_cache, value_cache, summary_keys, summary_values, owner_map, super_ids, fine_ids):
        own_rows, heads, head_dim = queries.shape
        groups, tokens = key_cache.shape[:2]
        requests = super_ids.shape[0]
        devices = seq_size * rep_size
        out_rows = own_rows // rep_size
        sources = math.gcd(seq_size, max(WIDTH // own_rows, 1))
        assert summary_keys.shape[1] == 1 and tokens == SUPER * BLK
        assert groups == 2 and heads == 8 and own_rows % rep_size == 0 and own_rows % 2 == 0
        assert requests % CHUNK == 0 and CHUNK % (sources * own_rows) == 0
        hbm = pl.BlockSpec(memory_space=pltpu.HBM)
        summary_keys = jnp.transpose(summary_keys, (1, 0, 2))
        summary_values = jnp.transpose(summary_values, (1, 0, 2))
        chunked = (requests // CHUNK, CHUNK, groups, -1)
        super_ids = jnp.transpose(super_ids.reshape(chunked), (0, 2, 3, 1))
        fine_ids = jnp.transpose(fine_ids.reshape(chunked), (0, 2, 3, 1))
        return pl.pallas_call(
            functools.partial(kernel, seq_size, rep_size),
            out_shape=pltpu.VMEM((out_rows, rep_size * heads, head_dim), jnp.bfloat16),
            in_specs=[hbm] * 8,
            out_specs=pl.BlockSpec(memory_space=pltpu.VMEM),
            scratch_shapes=[
                pltpu.VMEM(key_cache.shape, key_cache.dtype),
                pltpu.VMEM(value_cache.shape, value_cache.dtype),
                pltpu.VMEM(summary_keys.shape, summary_keys.dtype),
                pltpu.VMEM(summary_values.shape, summary_values.dtype),
                pltpu.SMEM(owner_map.shape, owner_map.dtype),
                pltpu.VMEM(super_ids.shape, super_ids.dtype),
                pltpu.VMEM(fine_ids.shape, fine_ids.dtype),
                pltpu.VMEM((seq_size * own_rows, heads, head_dim), jnp.bfloat16),
                pltpu.VMEM((requests, heads, head_dim), jnp.bfloat16),
                pltpu.VMEM((requests, 1, head_dim), jnp.float32),
                pltpu.VMEM((devices, out_rows, heads, head_dim), jnp.bfloat16),
                pltpu.VMEM((devices, out_rows, 1, head_dim), jnp.float32),
                pltpu.SemaphoreType.DMA((6,)),
                pltpu.SemaphoreType.DMA((2, groups)),
                pltpu.SemaphoreType.DMA,
                pltpu.SemaphoreType.DMA((seq_size // sources,)),
                pltpu.SemaphoreType.DMA((2,)),
                pltpu.SemaphoreType.DMA((2,)),
            ],
            compiler_params=pltpu.CompilerParams(collective_id=0, has_side_effects=True),
        )(queries, key_cache, value_cache, summary_keys, summary_values, owner_map, super_ids, fine_ids)

    in_specs = (
        P("seq", "rep", None),
        P("rep", "seq", None),
        P("rep", "seq", None),
        P("rep", "seq", None),
        P("rep", "seq", None),
        P(),
        P(None, "rep", None),
        P(None, "rep", None),
    )
    out_specs = P(("seq", "rep"), None, None)
    return jax.shard_map(shards, mesh=mesh, in_specs=in_specs, out_specs=out_specs, check_vma=False)
```

```python
import functools
import math

import jax
import jax.numpy as jnp
from jax import lax
from jax.experimental import pallas as pl
from jax.experimental.pallas import tpu as pltpu
from jax.sharding import PartitionSpec as P

BLK = 128
SUPER = 16
NEGATIVE = -1e30
LOG2E = math.log2(math.e)
CHUNK = 32
WIDTH = 16
UNROLL_LIMIT = 64


def repeat(count, body):
    if count <= UNROLL_LIMIT:
        for step in range(count):
            body(step)
    else:

        def rolled(step, carry):
            body(step)
            return carry

        lax.fori_loop(0, count, rolled, 0)


def kernel(
    seq_size,
    rep_size,
    q_hbm,
    k_hbm,
    v_hbm,
    sk_hbm,
    sv_hbm,
    owner_hbm,
    super_hbm,
    fine_hbm,
    out_ref,
    k_ref,
    v_ref,
    sk_ref,
    sv_ref,
    owner_ref,
    super_ref,
    fine_ref,
    q_all,
    part_values,
    landed_values,
    in_sems,
    kv_sems,
    q_send,
    q_recv,
    p_send,
    p_recv,
):
    my_seq = lax.axis_index("seq")
    my_rep = lax.axis_index("rep")
    devices = seq_size * rep_size
    own_rows, heads, head_dim = q_hbm.shape
    groups, tokens = k_ref.shape[:2]
    per_group = heads // groups
    slot_count = owner_ref.shape[0]
    out_rows = out_ref.shape[0]
    blocks = tokens // BLK
    near = q_recv.shape[0]
    sources = seq_size // near
    width = sources * own_rows
    my_block = lax.div(my_seq, sources)
    my_place = lax.rem(my_seq, sources)

    barrier = pltpu.get_barrier_semaphore()

    def reach(seq, rep):
        return dict(device_id=(seq, rep), device_id_type=pl.DeviceIdType.MESH)

    def greet_seq(step):
        pl.semaphore_signal(barrier, inc=1, **reach(lax.rem(my_seq + step + 1, seq_size), my_rep))

    def greet_rep(step):
        pl.semaphore_signal(barrier, inc=1, **reach(my_seq, lax.rem(my_rep + step + 1, rep_size)))

    repeat(seq_size - 1, greet_seq)
    repeat(rep_size - 1, greet_rep)

    mine = q_all.at[pl.ds(my_seq * own_rows, own_rows)]
    small = [
        pltpu.make_async_copy(src, dst, in_sems.at[i])
        for i, (src, dst) in enumerate(
            (
                (q_hbm, mine),
                (owner_hbm, owner_ref),
                (super_hbm, super_ref),
                (fine_hbm, fine_ref),
                (sk_hbm, sk_ref),
                (sv_hbm, sv_ref),
            )
        )
    ]
    for copy in small:
        copy.start()
    big = []
    for g in range(groups):
        big.append(pltpu.make_async_copy(k_hbm.at[g], k_ref.at[g], kv_sems.at[0, g]))
        big.append(pltpu.make_async_copy(v_hbm.at[g], v_ref.at[g], kv_sems.at[1, g]))
    for copy in big:
        copy.start()

    pl.semaphore_wait(barrier, seq_size - 1 + rep_size - 1)

    def send_query(away, place):
        block = lax.rem(my_block + away, near)
        pltpu.make_async_remote_copy(
            src_ref=q_hbm,
            dst_ref=mine,
            send_sem=q_send,
            recv_sem=q_recv.at[(near - away) % near],
            **reach(block * sources + place, my_rep),
        ).start()

    def send_block(step):
        away = near - 1 - step
        for place in range(sources):
            send_query(away, lax.rem(my_place + place, sources))

    repeat(near - 1, send_block)
    for place in range(1, sources):
        send_query(0, lax.rem(my_place + place, sources))

    for copy in small:
        copy.wait()

    if slot_count <= UNROLL_LIMIT:
        here = jnp.int32(0)
        for j in range(slot_count):
            here = here + jnp.where(owner_ref[j] == my_seq, j, 0)
    else:
        here = lax.fori_loop(
            0, slot_count, lambda j, total: total + jnp.where(owner_ref[j] == my_seq, j, 0), jnp.int32(0)
        )
    here = here.astype(jnp.float32)

    rows = width * per_group
    pairs = width // 2
    row_of = lax.broadcasted_iota(jnp.int32, (rows, CHUNK), 0)
    lane_of = lax.broadcasted_iota(jnp.int32, (rows, CHUNK), 1)
    scaling = head_dim ** (-0.5) * LOG2E
    sub = lax.broadcasted_iota(jnp.int32, (pairs, heads, head_dim), 1)
    lane = lax.broadcasted_iota(jnp.int32, (pairs, heads, head_dim), 2)
    top = sub < per_group

    def selection(first, g):
        chunk = lax.div(first, CHUNK)
        low = (lane_of - lax.rem(first, CHUNK)) * per_group
        expand = jnp.where((row_of >= low) & (row_of < low + per_group), 1.0, 0.0).astype(jnp.bfloat16)
        fine = fine_ref[chunk, g].astype(jnp.float32).astype(jnp.bfloat16)
        supers = super_ref[chunk, g].astype(jnp.float32).astype(jnp.bfloat16)
        contract = (((1,), (1,)), ((), ()))
        fine = lax.dot_general(expand, fine, contract, preferred_element_type=jnp.float32)
        supers = lax.dot_general(expand, supers, contract, preferred_element_type=jnp.float32)
        place = lax.broadcasted_iota(jnp.int32, supers.shape, 1).astype(jnp.float32) + 1.0
        place = jnp.sum(jnp.where(supers == here, place, 0.0), axis=1, keepdims=True)
        at = (fine - SUPER * (place - 1.0)).astype(jnp.int32)
        valid = (at >= 0) & (at < SUPER) & (place > 0.0)
        bit = jnp.left_shift(1, jnp.clip(at, 0, SUPER - 1)).astype(jnp.float32)
        bits = jnp.sum(jnp.where(valid, bit, 0.0), axis=1, keepdims=True).astype(jnp.int32)
        return place, bits

    def regroup(a, b):
        return jnp.where(top, a, pltpu.roll(b, per_group, 1)), jnp.where(top, pltpu.roll(a, per_group, 1), b)

    def attend(query, g, place, bits):
        bits = jnp.broadcast_to(bits, (rows, BLK))
        scores = lax.dot_general(
            query.astype(jnp.bfloat16), k_ref[g], (((1,), (1,)), ((), ())), preferred_element_type=jnp.float32
        )
        masked = []
        for b in range(blocks):
            one = scores[:, b * BLK : (b + 1) * BLK]
            masked.append(jnp.where((bits & (1 << b)) != 0, one, NEGATIVE))
        peak = functools.reduce(jnp.maximum, masked)
        peak = jnp.max(peak, axis=1, keepdims=True)
        weights = [jnp.exp2((one - peak) * scaling) for one in masked]
        total = jnp.sum(functools.reduce(jnp.add, weights), axis=1, keepdims=True)
        packed = jnp.concatenate([one.astype(jnp.bfloat16) for one in weights], axis=1)
        summed = jnp.dot(packed, v_ref[g], preferred_element_type=jnp.float32)
        coarse = jnp.sum(query * sk_ref[:, g].astype(jnp.float32), axis=1, keepdims=True)
        coarse = coarse * scaling + math.log2(SUPER)
        stat = jnp.where(place > 0.0, peak * scaling + jnp.log2(total), coarse)
        value = jnp.where(place > 0.0, summed / total, sv_ref[:, g].astype(jnp.float32))
        stat = jnp.broadcast_to(stat, (rows, head_dim))
        return value.reshape(pairs, heads, head_dim), stat.reshape(pairs, heads, head_dim)

    def block_parts(first, chosen):
        raw = q_all[pl.ds(first, width)].astype(jnp.float32).reshape(pairs, 2, heads, head_dim)
        queries = [one.reshape(rows, head_dim) for one in regroup(raw[:, 0], raw[:, 1])]
        (value_a, stat_a), (value_b, stat_b) = [attend(queries[g], g, *chosen[g]) for g in range(groups)]
        values = regroup(value_a, value_b)
        stats = regroup(stat_a, stat_b)
        for which in range(2):
            stat = stats[which]
            high = stat.astype(jnp.bfloat16).astype(jnp.float32)
            middle = (stat - high).astype(jnp.bfloat16).astype(jnp.float32)
            last = stat - high - middle
            split = jnp.where(lane == 0, high, jnp.where(lane == 1, middle, jnp.where(lane == 2, last, 0.0)))
            message = jnp.concatenate([values[which], split], axis=1).astype(jnp.bfloat16)
            for pair in range(pairs):
                part_values[first + 2 * pair + which] = message[pair]

    slot = pl.ds(my_rep * seq_size + my_seq, 1)
    messages = ((part_values, landed_values),)

    def send_parts(first, start, skip):
        targets = width // out_rows
        for step in range(skip, targets):
            target = lax.rem(start + step, targets)
            there = lax.div(first, out_rows) + target
            for kind, (source, landed) in enumerate(messages):
                pltpu.make_async_remote_copy(
                    src_ref=source.at[pl.ds(first + target * out_rows, out_rows)],
                    dst_ref=landed.at[my_rep * seq_size + my_seq],
                    send_sem=p_send.at[kind],
                    recv_sem=p_recv.at[kind],
                    **reach(lax.div(there, rep_size), lax.rem(there, rep_size)),
                ).start()

    def wait_block(away, count):
        got = q_all.at[pl.ds(0, count * own_rows)]
        pltpu.make_async_copy(got, got, q_recv.at[away]).wait()

    def block_first(away):
        return lax.rem(my_block + away, near) * width

    mine_at = my_place * rep_size + my_rep

    def run_block(away, chosen):
        wait_block(away, sources)
        block_parts(block_first(away), chosen)
        send_parts(block_first(away), mine_at, 0)

    def choose(away):
        return [selection(block_first(away), g) for g in range(groups)]

    ahead = [choose(away) for away in range(near)] if near <= 2 else None
    for copy in big:
        copy.wait()
    if sources > 1:
        wait_block(0, sources - 1)
    block_parts(block_first(0), ahead[0] if ahead else choose(0))
    send_parts(block_first(0), mine_at, 1)
    own = block_first(0) + mine_at * out_rows
    landed_values[slot] = part_values[pl.ds(own, out_rows)][None]

    if ahead:
        for away in range(1, near):
            run_block(away, ahead[away])
    else:

        def block_step(away, carry):
            run_block(away, choose(away))
            return carry

        lax.fori_loop(1, near, block_step, 0)

    for kind, (_, landed) in enumerate(messages):
        got = landed.at[pl.ds(0, devices - 1)]
        pltpu.make_async_copy(got, got, p_recv.at[kind]).wait()

    for i in range(out_rows):
        for p in range(rep_size):
            stats, values = [], []
            for s in range(seq_size):
                message = landed_values[p * seq_size + s, i].astype(jnp.float32)
                values.append(message[:heads])
                stats.append(jnp.sum(message[heads:], axis=1, keepdims=True))
            peak = functools.reduce(jnp.maximum, stats)
            factors = [jnp.exp2(stat - peak) for stat in stats]
            total = functools.reduce(jnp.add, factors)
            summed = functools.reduce(jnp.add, [f * v for f, v in zip(factors, values)])
            out_ref[i, p * heads : (p + 1) * heads] = (summed / total).astype(out_ref.dtype)

    sent = q_all.at[pl.ds(0, (seq_size - 1) * own_rows)]
    pltpu.make_async_copy(sent, sent, q_send).wait()
    for kind, (_, landed) in enumerate(messages):
        sent = landed.at[pl.ds(0, devices - 1)]
        pltpu.make_async_copy(sent, sent, p_send.at[kind]).wait()


def solution(mesh):
    seq_size = mesh.shape["seq"]
    rep_size = mesh.shape["rep"]

    def shards(queries, key_cache, value_cache, summary_keys, summary_values, owner_map, super_ids, fine_ids):
        own_rows, heads, head_dim = queries.shape
        groups, tokens = key_cache.shape[:2]
        requests = super_ids.shape[0]
        devices = seq_size * rep_size
        out_rows = own_rows // rep_size
        sources = math.gcd(seq_size, max(WIDTH // own_rows, 1))
        assert summary_keys.shape[1] == 1 and tokens == SUPER * BLK
        assert groups == 2 and heads == 8 and own_rows % rep_size == 0 and own_rows % 2 == 0
        assert requests % CHUNK == 0 and CHUNK % (sources * own_rows) == 0
        hbm = pl.BlockSpec(memory_space=pltpu.HBM)
        summary_keys = jnp.transpose(summary_keys, (1, 0, 2))
        summary_values = jnp.transpose(summary_values, (1, 0, 2))
        chunked = (requests // CHUNK, CHUNK, groups, -1)
        super_ids = jnp.transpose(super_ids.reshape(chunked), (0, 2, 3, 1))
        fine_ids = jnp.transpose(fine_ids.reshape(chunked), (0, 2, 3, 1))
        return pl.pallas_call(
            functools.partial(kernel, seq_size, rep_size),
            out_shape=pltpu.VMEM((out_rows, rep_size * heads, head_dim), jnp.bfloat16),
            in_specs=[hbm] * 8,
            out_specs=pl.BlockSpec(memory_space=pltpu.VMEM),
            scratch_shapes=[
                pltpu.VMEM(key_cache.shape, key_cache.dtype),
                pltpu.VMEM(value_cache.shape, value_cache.dtype),
                pltpu.VMEM(summary_keys.shape, summary_keys.dtype),
                pltpu.VMEM(summary_values.shape, summary_values.dtype),
                pltpu.SMEM(owner_map.shape, owner_map.dtype),
                pltpu.VMEM(super_ids.shape, super_ids.dtype),
                pltpu.VMEM(fine_ids.shape, fine_ids.dtype),
                pltpu.VMEM((seq_size * own_rows, heads, head_dim), jnp.bfloat16),
                pltpu.VMEM((requests, 2 * heads, head_dim), jnp.bfloat16),
                pltpu.VMEM((devices, out_rows, 2 * heads, head_dim), jnp.bfloat16),
                pltpu.SemaphoreType.DMA((6,)),
                pltpu.SemaphoreType.DMA((2, groups)),
                pltpu.SemaphoreType.DMA,
                pltpu.SemaphoreType.DMA((seq_size // sources,)),
                pltpu.SemaphoreType.DMA((2,)),
                pltpu.SemaphoreType.DMA((2,)),
            ],
            compiler_params=pltpu.CompilerParams(collective_id=0, has_side_effects=True),
        )(queries, key_cache, value_cache, summary_keys, summary_values, owner_map, super_ids, fine_ids)

    in_specs = (
        P("seq", "rep", None),
        P("rep", "seq", None),
        P("rep", "seq", None),
        P("rep", "seq", None),
        P("rep", "seq", None),
        P(),
        P(None, "rep", None),
        P(None, "rep", None),
    )
    out_specs = P(("seq", "rep"), None, None)
    return jax.shard_map(shards, mesh=mesh, in_specs=in_specs, out_specs=out_specs, check_vma=False)
```
